32 devices in a mesh: tm: 4 (over y, core), rows: 8 (over z, x).
Axes of the slice: x: 2, y: 2, z: 4, core: 2. Of those that a mesh axis runs over, the one named last changes fastest.
Arguments:
- features: bfloat16 [4, 24, 64, 512], P('tm', 'rows'), may hold values from -64 to 64, as said below
- gamma: float32 [512], replicated, may hold values from 0.1 to 1.9
- beta: float32 [512], replicated, may hold values from -3 to 3
- kernel: bfloat16 [3, 512, 3, 3, 512], P(None, 'tm'), may hold values from -0.0546875 to 0.0546875
- bias: float32 [512], replicated, may hold values from -3 to 3
Outputs:
- decoded: bfloat16 [4, 24, 64, 512], P('tm', 'rows')
The draws below stay inside these ranges and needn't reach their ends.
Inputs may be any that keep to these rules, and one draw needn't show every extreme that they name: features are finite.
All inputs are finite; a program needn't handle non-finite values.
Results may differ from the reference program's by a relative error of at most 0.004.
Values may be sent and summed in bfloat16 or wider, within the bound.
A program may use at most 128 MiB of HBM per device.

```python
import math
import jax
import jax.numpy as jnp
from jax import lax

C = 512
GROUPS = 32
WIDTH = 64
FRAMES = 4
HEIGHT = 24


def draw_features(key, part):
    first = jax.random.fold_in(key, 0)
    second = jax.random.fold_in(key, 1)
    fourth = jax.random.fold_in(key, 3)
    time_pos = jnp.arange(FRAMES, dtype=jnp.float32) / max(FRAMES - 1, 1)
    row_pos = jnp.arange(HEIGHT, dtype=jnp.float32) / max(HEIGHT - 1, 1)
    time_scale = 0.6 * jnp.exp(time_pos * math.log(3.0))
    row_scale = 0.6 * jnp.exp(row_pos * math.log(3.0))
    rising = time_scale[:, None, None, None] * row_scale[None, :, None, None]
    base = jnp.clip(jax.random.normal(first, (FRAMES, HEIGHT, WIDTH, C), jnp.float32), -6.0, 6.0)
    chan = jnp.exp(jax.random.uniform(second, (C,), jnp.float32, math.log(0.5), math.log(2.0)))
    offset = jax.random.uniform(fourth, (C,), jnp.float32, -1.5, 1.5)
    result = (base * chan + offset) * rising
    return result.astype(jnp.bfloat16)


def levels(key, extent, pieces, low, largest):
    loudness, own = 1.0, jax.random.fold_in(key, 6)
    for dim, blocks in pieces:
        heights = jnp.exp(jax.random.uniform(jax.random.fold_in(own, dim), (blocks,), jnp.float32, low / len(pieces), largest / len(pieces)))
        loudness = loudness * jnp.repeat(heights, extent[dim] // blocks).reshape([-1 if axis == dim else 1 for axis in range(len(extent))])
    return loudness


def scatter_about(own_key, dims, scale, bound, cuts=(), held_as=jnp.bfloat16):
    gain = levels(own_key, dims, cuts, -0.22, 0.18) if cuts else 1.0
    drawn = jax.random.normal(own_key, dims, jnp.float32) * scale * gain
    return jnp.minimum(jnp.maximum(drawn, -bound), bound).astype(held_as)


def setup_inputs(seed: int = 0) -> dict:
    splits = jax.random.split(jax.random.key(seed), 6)
    features = draw_features(jax.random.fold_in(splits[5], 71), 0)
    gamma = jnp.clip(1.0 + 0.18 * jax.random.normal(splits[1], (C,), jnp.float32), 0.1, 1.9)
    beta = scatter_about(splits[2], (C,), 0.5, 3.0, (), jnp.float32)
    kernel = scatter_about(splits[3], (3, C, 3, 3, C), (27 * C) ** -0.5, 0.0546875, ((1, 4),))
    bias = scatter_about(splits[4], (C,), 0.5, 3.0, (), jnp.float32)
    return dict(features=features, gamma=gamma, beta=beta, kernel=kernel, bias=bias)


def reference(features, gamma, beta, kernel, bias):
    frames, height, across, channels = features.shape
    values = features.astype(jnp.float32)
    grouped = values.reshape(frames, height, across, GROUPS, channels // GROUPS)
    center = lax.optimization_barrier(jnp.mean(grouped, axis=(0, 1, 2, 4)))
    centered = grouped - center[:, None]
    spread = lax.optimization_barrier(jnp.mean(centered * centered, axis=(0, 1, 2, 4)))
    normed = (centered * lax.rsqrt(spread + 1e-06)[:, None]).reshape(frames, height, across, channels)
    active = jax.nn.silu(normed * gamma + beta).astype(jnp.bfloat16)
    padded = jnp.concatenate([active[0:1], active[0:1], active], axis=0).astype(jnp.float32)
    taps = jnp.transpose(kernel.astype(jnp.float32), (0, 2, 3, 4, 1))
    conv = lax.conv_general_dilated(padded[None], taps, (1, 1, 1), ((0, 0), (1, 1), (1, 1)), dimension_numbers=('NDHWC', 'DHWIO', 'NDHWC'), precision=lax.Precision.HIGHEST, preferred_element_type=jnp.float32)[0]
    return (values + conv + bias).astype(jnp.bfloat16)
```

```python
import functools

import jax
import jax.numpy as jnp
from jax import lax
from jax.experimental import pallas as pl
from jax.experimental.pallas import tpu as pltpu
from jax.sharding import PartitionSpec as P

GROUPS = 32
EPSILON = 1e-06
LANES = 128
MESH = pl.DeviceIdType.MESH
CORES = 2


def group_sum(x, span):
    lane = lax.broadcasted_iota(jnp.int32, x.shape, 1)
    step = 1
    while step < span:
        upper = pltpu.roll(x, LANES - step, 1)
        lower = pltpu.roll(x, step, 1)
        x = x + jnp.where((lane & step) == 0, upper, lower)
        step *= 2
    return x


def body(nt, nr, features, gamma, beta, weights, bias, out, raw, xs, wp, w0, prod, stats,
         block, feat_sem, w_sem, stat_send, stat_recv, halo_send, sib_send, peer_send,
         recv, out_send, out_recv):
    ny = nt // CORES
    total = nt * nr
    _, height, across, channels = features.shape
    outs = weights.shape[3]
    chunks = channels // LANES
    span = channels // GROUPS
    tm = lax.axis_index("tm")
    row = lax.axis_index("rows")
    y = tm // CORES
    core = lax.rem(tm, CORES)
    sib = y * CORES + (1 - core)
    me = tm * nr + row
    pieces = ((0, 1), (1, height), (height + 1, 1))

    def tap_copies():
        for b in range(3):
            for c in range(3):
                cols = pl.ds(c * channels, channels)
                yield pltpu.make_async_copy(weights.at[0, b, c], w0.at[b, :, cols], w_sem.at[0])
                for a in (1, 2):
                    yield pltpu.make_async_copy(
                        weights.at[a, b, c], wp.at[b, pl.ds((a - 1) * outs, outs), cols],
                        w_sem.at[1])

    own = pltpu.make_async_copy(features, raw.at[pl.ds(tm, 1), pl.ds(1, height)], feat_sem)
    own.start()
    barrier = pltpu.get_barrier_semaphore()

    def greet(i, carry):
        other = lax.rem(me + i, total)
        pl.semaphore_signal(barrier, inc=1, device_id=(other // nr, lax.rem(other, nr)),
                            device_id_type=MESH)
        return carry

    lax.fori_loop(1, total, greet, 0)
    for copy in tap_copies():
        copy.start()
    own.wait()

    values = raw[tm, 1:1 + height].astype(jnp.float32).reshape(height * across, channels)
    count = float(height * across * span)
    sums = jnp.sum(values, axis=0, keepdims=True)
    rows8 = jnp.concatenate([sums[:, i * LANES:(i + 1) * LANES] for i in range(chunks)], axis=0)
    means = group_sum(rows8, span) * (1.0 / count)
    wide = jnp.concatenate([means[i:i + 1] for i in range(chunks)], axis=1)
    centred = values - wide
    squares = jnp.sum(centred * centred, axis=0, keepdims=True)
    rows8 = jnp.concatenate([squares[:, i * LANES:(i + 1) * LANES] for i in range(chunks)], axis=0)
    moments = group_sum(rows8, span)
    place = lax.broadcasted_iota(jnp.int32, (1, LANES), 1) % span
    packed = jnp.zeros((1, LANES), jnp.float32)
    for i in range(chunks):
        packed = jnp.where(place == i, means[i:i + 1], packed)
        packed = jnp.where(place == chunks + i, moments[i:i + 1], packed)
    stats[me] = packed

    pl.semaphore_wait(barrier, total - 1)

    def stat_copy(i):
        other = lax.rem(me + i, total)
        return pltpu.make_async_remote_copy(
            src_ref=stats.at[me], dst_ref=stats.at[me], send_sem=stat_send, recv_sem=stat_recv,
            device_id=(other // nr, lax.rem(other, nr)), device_id_type=MESH)

    def send_stat(i, carry):
        stat_copy(i).start()
        return carry

    lax.fori_loop(1, total, send_stat, 0)

    def piece(f, p):
        first, size = pieces[p]
        return raw.at[f, pl.ds(first, size)]

    def to_sib(f, p):
        return pltpu.make_async_remote_copy(
            src_ref=piece(f, p), dst_ref=piece(f, p), send_sem=sib_send.at[f, p],
            recv_sem=recv.at[f, p], device_id=(sib, row), device_id_type=MESH)

    def to_peer(d, p):
        other = lax.rem(y + d, ny) * CORES + core
        return pltpu.make_async_remote_copy(
            src_ref=piece(tm, p), dst_ref=piece(tm, p), send_sem=peer_send.at[d, p],
            recv_sem=recv.at[tm, p], device_id=(other, row), device_id_type=MESH)

    def from_any(f, p):
        return pltpu.make_async_remote_copy(
            src_ref=piece(f, p), dst_ref=piece(f, p), send_sem=sib_send.at[f, p],
            recv_sem=recv.at[f, p], device_id=(sib, row), device_id_type=MESH)

    up_copy = pltpu.make_async_remote_copy(
        src_ref=raw.at[tm, pl.ds(height, 1)], dst_ref=raw.at[tm, pl.ds(0, 1)],
        send_sem=halo_send.at[0], recv_sem=recv.at[tm, 0],
        device_id=(tm, jnp.minimum(row + 1, nr - 1)), device_id_type=MESH)
    down_copy = pltpu.make_async_remote_copy(
        src_ref=raw.at[tm, pl.ds(1, 1)], dst_ref=raw.at[tm, pl.ds(height + 1, 1)],
        send_sem=halo_send.at[1], recv_sem=recv.at[tm, 2],
        device_id=(tm, jnp.maximum(row - 1, 0)), device_id_type=MESH)
    has_above = row > 0
    has_below = row < nr - 1

    @pl.when(has_below)
    def _():
        up_copy.start()

    @pl.when(has_above)
    def _():
        down_copy.start()

    def loop_peers(fn):
        def step(d, carry):
            fn(d)
            return carry
        lax.fori_loop(1, ny, step, 0)

    loop_peers(lambda d: to_peer(d, 1).start())
    to_sib(tm, 1).start()

    for p, there in ((0, has_above), (2, has_below)):
        @pl.when(there)
        def _(p=p):
            from_any(tm, p).wait_recv()
            loop_peers(lambda d: to_peer(d, p).start())
            to_sib(tm, p).start()

    pltpu.make_async_remote_copy(
        src_ref=stats.at[pl.ds(0, total - 1)], dst_ref=stats.at[pl.ds(0, total - 1)],
        send_sem=stat_send, recv_sem=stat_recv, device_id=(sib, row),
        device_id_type=MESH).wait()
    every = stats[...].reshape(total, LANES)
    summed = jnp.sum(every, axis=0, keepdims=True)
    middle = summed * (1.0 / total)
    away = every - middle
    away = jnp.sum(away * away, axis=0, keepdims=True) * count
    rows = []
    for i in range(chunks):
        rows.append(jnp.where(place == i, middle, 0.0))
    for i in range(chunks):
        rows.append(jnp.where(place == chunks + i, summed, 0.0)
                    + jnp.where(place == i, away, 0.0))
    spread_out = group_sum(jnp.concatenate(rows, axis=0), span)
    center = jnp.concatenate([spread_out[i:i + 1] for i in range(chunks)], axis=1)
    spread = jnp.concatenate(
        [spread_out[chunks + i:chunks + i + 1] for i in range(chunks)], axis=1)
    spread = spread * (1.0 / (count * total))
    gain = lax.rsqrt(spread + EPSILON) * gamma[...]
    shift = beta[...]

    column = lax.broadcasted_iota(jnp.int32, (across, channels), 0)

    def activate_row(f, i):
        v = (raw[f, i].astype(jnp.float32) - center) * gain + shift
        v = v * 0.5
        v = v * jnp.tanh(v) + v
        before = jnp.where(column == 0, 0.0, pltpu.roll(v, 1, 0))
        after = jnp.where(column == across - 1, 0.0, pltpu.roll(v, across - 1, 0))
        xs[f, i, :, 0:channels] = before.astype(jnp.bfloat16)
        xs[f, i, :, channels:2 * channels] = v.astype(jnp.bfloat16)
        xs[f, i, :, 2 * channels:] = after.astype(jnp.bfloat16)

    def edge_row(f, i, there):
        @pl.when(there)
        def _():
            activate_row(f, i)

        @pl.when(jnp.logical_not(there))
        def _():
            xs[f, i] = jnp.zeros((across, 3 * channels), jnp.bfloat16)

    def dot(f, taps, b):
        left = xs[f, b:b + height].reshape(height * across, 3 * channels)
        return lax.dot_general(left, taps[b], (((1,), (1,)), ((), ())),
                               preferred_element_type=jnp.float32)

    def process(f):
        for i in range(1, height + 1):
            activate_row(f, i)
        edge_row(f, 0, has_above)
        edge_row(f, height + 1, has_below)
        pair = dot(f, wp, 0) + dot(f, wp, 1) + dot(f, wp, 2)
        prod[f, 1] = pair[:, 0:outs]
        prod[f, 2] = pair[:, outs:2 * outs]

        @pl.when(jnp.logical_or(f == 0, f + 2 < nt))
        def _():
            prod[f, 0] = dot(f, w0, 0) + dot(f, w0, 1) + dot(f, w0, 2)

    def wait_frame(f, forward):
        from_any(f, 1).wait_recv()
        if forward:
            to_sib(f, 1).start()
        for p, there in ((0, has_above), (2, has_below)):
            @pl.when(there)
            def _(p=p):
                from_any(f, p).wait_recv()
                if forward:
                    to_sib(f, p).start()

    pltpu.make_async_copy(w0, w0, w_sem.at[0]).wait()
    pltpu.make_async_copy(wp, wp, w_sem.at[1]).wait()
    process(tm)
    wait_frame(sib, False)
    process(sib)

    def far(d):
        base = lax.rem(y + d, ny) * CORES
        wait_frame(base + core, True)
        process(base + core)
        wait_frame(base + 1 - core, False)
        process(base + 1 - core)

    loop_peers(far)

    def lanes_of(x):
        if outs % LANES == 0:
            return x[..., pl.ds(pl.multiple_of(tm * outs, LANES), outs)]
        full = x[...].astype(jnp.float32)
        full = full.reshape(-1, channels)
        moved = pltpu.roll(full, channels - tm * outs, 1)
        return moved[:, 0:outs]

    if outs % LANES == 0:
        offset = lanes_of(bias)
    else:
        offset = lanes_of(jnp.broadcast_to(bias[...], (8, channels)))[0:1]

    def out_copy(f):
        return pltpu.make_async_remote_copy(
            src_ref=block.at[f], dst_ref=out.at[tm], send_sem=out_send.at[f],
            recv_sem=out_recv.at[tm], device_id=(f, row), device_id_type=MESH)

    def finish(f):
        conv = (prod[f, 2] + prod[jnp.maximum(f - 1, 0), 1]) + prod[jnp.maximum(f - 2, 0), 0]
        kept = lanes_of(raw.at[f, 1:1 + height]).astype(jnp.float32)
        kept = kept.reshape(height * across, outs)
        return (kept + conv + offset).astype(jnp.bfloat16)

    def give(f):
        block[f] = finish(f)
        out_copy(f).start()

    def give_far(d):
        base = lax.rem(y + d, ny) * CORES
        give(base + core)
        give(base + 1 - core)

    loop_peers(give_far)
    give(sib)
    out[tm] = finish(tm)

    def take(i, carry):
        src = lax.rem(tm + i, nt)
        pltpu.make_async_remote_copy(
            src_ref=block.at[src], dst_ref=out.at[src], send_sem=out_send.at[src],
            recv_sem=out_recv.at[src], device_id=(sib, row), device_id_type=MESH).wait()
        return carry

    lax.fori_loop(1, nt, take, 0)

    @pl.when(has_below)
    def _():
        up_copy.wait_send()

    @pl.when(has_above)
    def _():
        down_copy.wait_send()

    for p, there in ((0, has_above), (1, None), (2, has_below)):
        def drain(p=p):
            def one(d):
                to_peer(d, p).wait_send()
                to_sib(lax.rem(y + d, ny) * CORES + core, p).wait_send()
            loop_peers(one)
            to_sib(tm, p).wait_send()
        if there is None:
            drain()
        else:
            pl.when(there)(drain)


def local(nt, nr, features, gamma, beta, kernel, bias):
    _, height, across, channels = features.shape
    outs = kernel.shape[1]
    total = nt * nr
    weights = jnp.transpose(kernel, (0, 2, 3, 1, 4))
    vmem = pl.BlockSpec(memory_space=pltpu.VMEM)
    anywhere = pl.BlockSpec(memory_space=pl.ANY)
    bf16, f32 = jnp.bfloat16, jnp.float32
    dma = pltpu.SemaphoreType.DMA
    parts = pl.pallas_call(
        functools.partial(body, nt, nr),
        out_shape=jax.ShapeDtypeStruct((nt, height * across, outs), bf16),
        in_specs=[anywhere, vmem, vmem, anywhere, vmem],
        out_specs=vmem,
        scratch_shapes=[
            pltpu.VMEM((nt, height + 2, across, channels), bf16),
            pltpu.VMEM((nt, height + 2, across, 3 * channels), bf16),
            pltpu.VMEM((3, 2 * outs, 3 * channels), bf16),
            pltpu.VMEM((3, outs, 3 * channels), bf16),
            pltpu.VMEM((nt, 3, height * across, outs), f32),
            pltpu.VMEM((total, 1, LANES), f32),
            pltpu.VMEM((nt, height * across, outs), bf16),
            dma, dma((2,)), dma, dma,
            dma((2,)), dma((nt, 3)), dma((nt // CORES, 3)), dma((nt, 3)),
            dma((nt,)), dma((nt,)),
        ],
        compiler_params=pltpu.CompilerParams(collective_id=0, has_side_effects=True),
    )(features, gamma.reshape(1, -1), beta.reshape(1, -1), weights, bias.reshape(1, -1))
    return jnp.transpose(parts, (1, 0, 2)).reshape(features.shape)


def solution(mesh):
    nt, nr = mesh.shape["tm"], mesh.shape["rows"]
    in_specs = (P("tm", "rows", None, None), P(), P(), P(None, "tm", None, None, None), P())
    out_specs = P("tm", "rows", None, None)
    return jax.shard_map(functools.partial(local, nt, nr), mesh=mesh, in_specs=in_specs,
                         out_specs=out_specs, check_vma=False)
```

```python
import functools

import jax
import jax.numpy as jnp
from jax import lax
from jax.experimental import pallas as pl
from jax.experimental.pallas import tpu as pltpu
from jax.sharding import PartitionSpec as P

GROUPS = 32
EPSILON = 1e-06
LANES = 128
MESH = pl.DeviceIdType.MESH
CORES = 2


def group_sum(x, span):
    lane = lax.broadcasted_iota(jnp.int32, x.shape, 1)
    step = 1
    while step < span:
        upper = pltpu.roll(x, LANES - step, 1)
        lower = pltpu.roll(x, step, 1)
        x = x + jnp.where((lane & step) == 0, upper, lower)
        step *= 2
    return x


def body(nt, nr, features, gamma, beta, weights, bias, out, raw, xs, wp, w0, prod, stats,
         block, feat_sem, w_sem, stat_send, stat_recv, halo_send, sib_send, peer_send,
         recv, out_send, out_recv):
    ny = nt // CORES
    total = nt * nr
    _, height, across, channels = features.shape
    outs = weights.shape[3]
    chunks = channels // LANES
    span = channels // GROUPS
    tm = lax.axis_index("tm")
    row = lax.axis_index("rows")
    y = tm // CORES
    core = lax.rem(tm, CORES)
    sib = y * CORES + (1 - core)
    me = tm * nr + row
    pieces = ((0, 1), (1, height), (height + 1, 1))

    def tap_copies():
        for b in range(3):
            for c in range(3):
                cols = pl.ds(c * channels, channels)
                yield pltpu.make_async_copy(weights.at[0, b, c], w0.at[b, :, cols], w_sem.at[0])
                for a in (1, 2):
                    yield pltpu.make_async_copy(
                        weights.at[a, b, c], wp.at[b, pl.ds((a - 1) * outs, outs), cols],
                        w_sem.at[1])

    own = pltpu.make_async_copy(features, raw.at[pl.ds(tm, 1), pl.ds(1, height)], feat_sem)
    own.start()
    barrier = pltpu.get_barrier_semaphore()

    def greet(i, carry):
        other = lax.rem(me + i, total)
        pl.semaphore_signal(barrier, inc=1, device_id=(other // nr, lax.rem(other, nr)),
                            device_id_type=MESH)
        return carry

    lax.fori_loop(1, total, greet, 0)
    for copy in tap_copies():
        copy.start()
    own.wait()

    values = raw[tm, 1:1 + height].astype(jnp.float32).reshape(height * across, channels)
    count = float(height * across * span)
    sums = jnp.sum(values, axis=0, keepdims=True)
    rows8 = jnp.concatenate([sums[:, i * LANES:(i + 1) * LANES] for i in range(chunks)], axis=0)
    means = group_sum(rows8, span) * (1.0 / count)
    wide = jnp.concatenate([means[i:i + 1] for i in range(chunks)], axis=1)
    centred = values - wide
    squares = jnp.sum(centred * centred, axis=0, keepdims=True)
    rows8 = jnp.concatenate([squares[:, i * LANES:(i + 1) * LANES] for i in range(chunks)], axis=0)
    moments = group_sum(rows8, span)
    place = lax.broadcasted_iota(jnp.int32, (1, LANES), 1) % span
    packed = jnp.zeros((1, LANES), jnp.float32)
    for i in range(chunks):
        packed = jnp.where(place == i, means[i:i + 1], packed)
        packed = jnp.where(place == chunks + i, moments[i:i + 1], packed)
    stats[me] = packed

    pl.semaphore_wait(barrier, total - 1)

    def stat_copy(i):
        other = lax.rem(me + i, total)
        return pltpu.make_async_remote_copy(
            src_ref=stats.at[me], dst_ref=stats.at[me], send_sem=stat_send, recv_sem=stat_recv,
            device_id=(other // nr, lax.rem(other, nr)), device_id_type=MESH)

    def send_stat(i, carry):
        stat_copy(i).start()
        return carry

    lax.fori_loop(1, total, send_stat, 0)

    def piece(f, p):
        first, size = pieces[p]
        return raw.at[f, pl.ds(first, size)]

    def to_sib(f, p):
        return pltpu.make_async_remote_copy(
            src_ref=piece(f, p), dst_ref=piece(f, p), send_sem=sib_send.at[f, p],
            recv_sem=recv.at[f, p], device_id=(sib, row), device_id_type=MESH)

    def to_peer(d, p):
        other = lax.rem(y + d, ny) * CORES + core
        return pltpu.make_async_remote_copy(
            src_ref=piece(tm, p), dst_ref=piece(tm, p), send_sem=peer_send.at[d, p],
            recv_sem=recv.at[tm, p], device_id=(other, row), device_id_type=MESH)

    def from_any(f, p):
        return pltpu.make_async_remote_copy(
            src_ref=piece(f, p), dst_ref=piece(f, p), send_sem=sib_send.at[f, p],
            recv_sem=recv.at[f, p], device_id=(sib, row), device_id_type=MESH)

    up_copy = pltpu.make_async_remote_copy(
        src_ref=raw.at[tm, pl.ds(height, 1)], dst_ref=raw.at[tm, pl.ds(0, 1)],
        send_sem=halo_send.at[0], recv_sem=recv.at[tm, 0],
        device_id=(tm, jnp.minimum(row + 1, nr - 1)), device_id_type=MESH)
    down_copy = pltpu.make_async_remote_copy(
        src_ref=raw.at[tm, pl.ds(1, 1)], dst_ref=raw.at[tm, pl.ds(height + 1, 1)],
        send_sem=halo_send.at[1], recv_sem=recv.at[tm, 2],
        device_id=(tm, jnp.maximum(row - 1, 0)), device_id_type=MESH)
    has_above = row > 0
    has_below = row < nr - 1

    @pl.when(has_below)
    def _():
        up_copy.start()

    @pl.when(has_above)
    def _():
        down_copy.start()

    def loop_peers(fn):
        def step(d, carry):
            fn(d)
            return carry
        lax.fori_loop(1, ny, step, 0)

    loop_peers(lambda d: to_peer(d, 1).start())
    to_sib(tm, 1).start()

    for p, there in ((0, has_above), (2, has_below)):
        @pl.when(there)
        def _(p=p):
            from_any(tm, p).wait_recv()
            loop_peers(lambda d: to_peer(d, p).start())
            to_sib(tm, p).start()

    pltpu.make_async_remote_copy(
        src_ref=stats.at[pl.ds(0, total - 1)], dst_ref=stats.at[pl.ds(0, total - 1)],
        send_sem=stat_send, recv_sem=stat_recv, device_id=(sib, row),
        device_id_type=MESH).wait()
    every = stats[...].reshape(total, LANES)
    summed = jnp.sum(every, axis=0, keepdims=True)
    middle = summed * (1.0 / total)
    away = every - middle
    away = jnp.sum(away * away, axis=0, keepdims=True) * count
    rows = []
    for i in range(chunks):
        rows.append(jnp.where(place == i, middle, 0.0))
    for i in range(chunks):
        rows.append(jnp.where(place == chunks + i, summed, 0.0)
                    + jnp.where(place == i, away, 0.0))
    spread_out = group_sum(jnp.concatenate(rows, axis=0), span)
    center = jnp.concatenate([spread_out[i:i + 1] for i in range(chunks)], axis=1)
    spread = jnp.concatenate(
        [spread_out[chunks + i:chunks + i + 1] for i in range(chunks)], axis=1)
    spread = spread * (1.0 / (count * total))
    gain = lax.rsqrt(spread + EPSILON) * gamma[...]
    shift = beta[...]

    column = lax.broadcasted_iota(jnp.int32, (across, channels), 0)

    def activate_row(f, i, there=None):
        v = (raw[f, i].astype(jnp.float32) - center) * gain + shift
        v = v * 0.5
        v = v * jnp.tanh(v) + v
        if there is not None:
            v = jnp.where(there, v, 0.0)
        before = jnp.where(column == 0, 0.0, pltpu.roll(v, 1, 0))
        after = jnp.where(column == across - 1, 0.0, pltpu.roll(v, across - 1, 0))
        xs[f, i, :, 0:channels] = before.astype(jnp.bfloat16)
        xs[f, i, :, channels:2 * channels] = v.astype(jnp.bfloat16)
        xs[f, i, :, 2 * channels:] = after.astype(jnp.bfloat16)

    def activate(f):
        activate_row(f, 0, has_above)
        for i in range(1, height + 1):
            activate_row(f, i)
        activate_row(f, height + 1, has_below)

    def dot(base, taps):
        total_out = None
        for b in range(3):
            left = xs[pl.ds(base, CORES), b:b + height]
            left = left.reshape(CORES * height * across, 3 * channels)
            part = lax.dot_general(left, taps[b], (((1,), (1,)), ((), ())),
                                   preferred_element_type=jnp.float32)
            total_out = part if total_out is None else total_out + part
        return total_out.reshape(CORES, height, across, -1)

    def convolve(base):
        pair = dot(base, wp)
        prod[1, pl.ds(base, CORES)] = pair[..., 0:outs]
        prod[2, pl.ds(base, CORES)] = pair[..., outs:2 * outs]

        @pl.when(jnp.logical_or(base == 0, base + 2 < nt))
        def _():
            prod[0, pl.ds(base, CORES)] = dot(base, w0)

    def wait_frame(f, forward):
        from_any(f, 1).wait_recv()
        if forward:
            to_sib(f, 1).start()
        for p, there in ((0, has_above), (2, has_below)):
            @pl.when(there)
            def _(p=p):
                from_any(f, p).wait_recv()
                if forward:
                    to_sib(f, p).start()

    pltpu.make_async_copy(w0, w0, w_sem.at[0]).wait()
    pltpu.make_async_copy(wp, wp, w_sem.at[1]).wait()
    activate(tm)
    wait_frame(sib, False)
    activate(sib)
    convolve(y * CORES)

    def far(d):
        base = lax.rem(y + d, ny) * CORES
        wait_frame(base + core, True)
        activate(base + core)
        wait_frame(base + 1 - core, False)
        activate(base + 1 - core)
        convolve(base)

    loop_peers(far)

    direct = outs % LANES == 0

    def lanes_of(x):
        if direct:
            return x[..., pl.ds(pl.multiple_of(tm * outs, LANES), outs)]
        full = x[...].astype(jnp.float32)
        lead = full.shape[:-1]
        moved = pltpu.roll(full.reshape(-1, channels), channels - tm * outs, 1)
        return moved[:, 0:outs].reshape(*lead, outs)

    if direct:
        offset = lanes_of(bias)
    else:
        offset = lanes_of(jnp.broadcast_to(bias[...], (8, channels)))[0:1]

    def landing(src):
        if direct:
            return out.at[0, :, :, pl.ds(pl.multiple_of(src * outs, LANES), outs)]
        return out.at[src]

    def out_copy(f):
        return pltpu.make_async_remote_copy(
            src_ref=block.at[f], dst_ref=landing(tm), send_sem=out_send.at[f],
            recv_sem=out_recv.at[tm], device_id=(f, row), device_id_type=MESH)

    def finish(f):
        conv = (prod[2, f] + prod[1, jnp.maximum(f - 1, 0)]) + prod[0, jnp.maximum(f - 2, 0)]
        kept = lanes_of(raw.at[f, 1:1 + height]).astype(jnp.float32)
        return (kept + conv + offset).astype(jnp.bfloat16)

    def give(f):
        block[f] = finish(f)
        out_copy(f).start()

    def give_far(d):
        base = lax.rem(y + d, ny) * CORES
        give(base + core)
        give(base + 1 - core)

    loop_peers(give_far)
    give(sib)
    if direct:
        out[0, :, :, pl.ds(pl.multiple_of(tm * outs, LANES), outs)] = finish(tm)
    else:
        out[tm] = finish(tm)

    def take(i, carry):
        src = lax.rem(tm + i, nt)
        pltpu.make_async_remote_copy(
            src_ref=block.at[src], dst_ref=landing(src), send_sem=out_send.at[src],
            recv_sem=out_recv.at[src], device_id=(sib, row), device_id_type=MESH).wait()
        return carry

    lax.fori_loop(1, nt, take, 0)

    @pl.when(has_below)
    def _():
        up_copy.wait_send()

    @pl.when(has_above)
    def _():
        down_copy.wait_send()

    for p, there in ((0, has_above), (1, None), (2, has_below)):
        def drain(p=p):
            def one(d):
                to_peer(d, p).wait_send()
                to_sib(lax.rem(y + d, ny) * CORES + core, p).wait_send()
            loop_peers(one)
            to_sib(tm, p).wait_send()
        if there is None:
            drain()
        else:
            pl.when(there)(drain)


def local(nt, nr, features, gamma, beta, kernel, bias):
    _, height, across, channels = features.shape
    outs = kernel.shape[1]
    total = nt * nr
    weights = jnp.transpose(kernel, (0, 2, 3, 1, 4))
    direct = outs % LANES == 0
    shape = features.shape if direct else (nt, height, across, outs)
    vmem = pl.BlockSpec(memory_space=pltpu.VMEM)
    anywhere = pl.BlockSpec(memory_space=pl.ANY)
    bf16, f32 = jnp.bfloat16, jnp.float32
    dma = pltpu.SemaphoreType.DMA
    parts = pl.pallas_call(
        functools.partial(body, nt, nr),
        out_shape=jax.ShapeDtypeStruct(shape, bf16),
        in_specs=[anywhere, vmem, vmem, anywhere, vmem],
        out_specs=vmem,
        scratch_shapes=[
            pltpu.VMEM((nt, height + 2, across, channels), bf16),
            pltpu.VMEM((nt, height + 2, across, 3 * channels), bf16),
            pltpu.VMEM((3, 2 * outs, 3 * channels), bf16),
            pltpu.VMEM((3, outs, 3 * channels), bf16),
            pltpu.VMEM((3, nt, height, across, outs), f32),
            pltpu.VMEM((total, 1, LANES), f32),
            pltpu.VMEM((nt, height, across, outs), bf16),
            dma, dma((2,)), dma, dma,
            dma((2,)), dma((nt, 3)), dma((nt // CORES, 3)), dma((nt, 3)),
            dma((nt,)), dma((nt,)),
        ],
        compiler_params=pltpu.CompilerParams(collective_id=0, has_side_effects=True),
    )(features, gamma.reshape(1, -1), beta.reshape(1, -1), weights, bias.reshape(1, -1))
    if direct:
        return parts
    return jnp.transpose(parts, (1, 2, 0, 3)).reshape(features.shape)


def solution(mesh):
    nt, nr = mesh.shape["tm"], mesh.shape["rows"]
    in_specs = (P("tm", "rows", None, None), P(), P(), P(None, "tm", None, None, None), P())
    out_specs = P("tm", "rows", None, None)
    return jax.shard_map(functools.partial(local, nt, nr), mesh=mesh, in_specs=in_specs,
                         out_specs=out_specs, check_vma=False)
```

```python
import functools

import jax
import jax.numpy as jnp
from jax import lax
from jax.experimental import pallas as pl
from jax.experimental.pallas import tpu as pltpu
from jax.sharding import PartitionSpec as P

GROUPS = 32
EPSILON = 1e-06
LANES = 128
MESH = pl.DeviceIdType.MESH
CORES = 2
VMEM_LIMIT = 67043328 - 262144


def group_sum(x, span):
    lane = lax.broadcasted_iota(jnp.int32, x.shape, 1)
    step = 1
    while step < span:
        upper = pltpu.roll(x, LANES - step, 1)
        lower = pltpu.roll(x, step, 1)
        x = x + jnp.where((lane & step) == 0, upper, lower)
        step *= 2
    return x


def body(nt, nr, features, gamma, beta, weights, bias, out, raw, xs, wp, w0, prod, stats,
         block, feat_sem, w_sem, stat_send, stat_recv, halo_send, sib_send, peer_send,
         recv, out_send, out_recv):
    ny = nt // CORES
    total = nt * nr
    _, height, across, channels = features.shape
    outs = weights.shape[3]
    chunks = channels // LANES
    span = channels // GROUPS
    tm = lax.axis_index("tm")
    row = lax.axis_index("rows")
    y = tm // CORES
    core = lax.rem(tm, CORES)
    sib = y * CORES + (1 - core)
    me = tm * nr + row
    pieces = ((0, 1), (1, height), (height + 1, 1))

    def tap_copies():
        for b in range(3):
            for c in range(3):
                cols = pl.ds(c * channels, channels)
                yield pltpu.make_async_copy(weights.at[0, b, c], w0.at[b, :, cols], w_sem.at[0])
                for a in (1, 2):
                    yield pltpu.make_async_copy(
                        weights.at[a, b, c], wp.at[b, pl.ds((a - 1) * outs, outs), cols],
                        w_sem.at[1])

    own = pltpu.make_async_copy(features, raw.at[pl.ds(tm, 1), pl.ds(1, height)], feat_sem)
    own.start()
    barrier = pltpu.get_barrier_semaphore()

    def greet(i, carry):
        other = lax.rem(me + i, total)
        pl.semaphore_signal(barrier, inc=1, device_id=(other // nr, lax.rem(other, nr)),
                            device_id_type=MESH)
        return carry

    lax.fori_loop(1, total, greet, 0)
    for copy in tap_copies():
        copy.start()
    own.wait()

    values = raw[tm, 1:1 + height].astype(jnp.float32).reshape(height * across, channels)
    count = float(height * across * span)
    sums = jnp.sum(values, axis=0, keepdims=True)
    rows8 = jnp.concatenate([sums[:, i * LANES:(i + 1) * LANES] for i in range(chunks)], axis=0)
    means = group_sum(rows8, span) * (1.0 / count)
    wide = jnp.concatenate([means[i:i + 1] for i in range(chunks)], axis=1)
    centred = values - wide
    squares = jnp.sum(centred * centred, axis=0, keepdims=True)
    rows8 = jnp.concatenate([squares[:, i * LANES:(i + 1) * LANES] for i in range(chunks)], axis=0)
    moments = group_sum(rows8, span)
    place = lax.broadcasted_iota(jnp.int32, (1, LANES), 1) % span
    packed = jnp.zeros((1, LANES), jnp.float32)
    for i in range(chunks):
        packed = jnp.where(place == i, means[i:i + 1], packed)
        packed = jnp.where(place == chunks + i, moments[i:i + 1], packed)
    stats[me] = packed

    pl.semaphore_wait(barrier, total - 1)

    def stat_copy(i):
        other = lax.rem(me + i, total)
        return pltpu.make_async_remote_copy(
            src_ref=stats.at[me], dst_ref=stats.at[me], send_sem=stat_send, recv_sem=stat_recv,
            device_id=(other // nr, lax.rem(other, nr)), device_id_type=MESH)

    def send_stat(i, carry):
        stat_copy(i).start()
        return carry

    lax.fori_loop(1, total, send_stat, 0)

    def piece(f, p):
        first, size = pieces[p]
        return raw.at[f, pl.ds(first, size)]

    def to_sib(f, p):
        return pltpu.make_async_remote_copy(
            src_ref=piece(f, p), dst_ref=piece(f, p), send_sem=sib_send.at[f, p],
            recv_sem=recv.at[f, p], device_id=(sib, row), device_id_type=MESH)

    def to_peer(d, p):
        other = lax.rem(y + d, ny) * CORES + core
        return pltpu.make_async_remote_copy(
            src_ref=piece(tm, p), dst_ref=piece(tm, p), send_sem=peer_send.at[d, p],
            recv_sem=recv.at[tm, p], device_id=(other, row), device_id_type=MESH)

    def from_any(f, p):
        return pltpu.make_async_remote_copy(
            src_ref=piece(f, p), dst_ref=piece(f, p), send_sem=sib_send.at[f, p],
            recv_sem=recv.at[f, p], device_id=(sib, row), device_id_type=MESH)

    up_copy = pltpu.make_async_remote_copy(
        src_ref=raw.at[tm, pl.ds(height, 1)], dst_ref=raw.at[tm, pl.ds(0, 1)],
        send_sem=halo_send.at[0], recv_sem=recv.at[tm, 0],
        device_id=(tm, jnp.minimum(row + 1, nr - 1)), device_id_type=MESH)
    down_copy = pltpu.make_async_remote_copy(
        src_ref=raw.at[tm, pl.ds(1, 1)], dst_ref=raw.at[tm, pl.ds(height + 1, 1)],
        send_sem=halo_send.at[1], recv_sem=recv.at[tm, 2],
        device_id=(tm, jnp.maximum(row - 1, 0)), device_id_type=MESH)
    has_above = row > 0
    has_below = row < nr - 1

    @pl.when(has_below)
    def _():
        up_copy.start()

    @pl.when(has_above)
    def _():
        down_copy.start()

    def loop_peers(fn):
        def step(d, carry):
            fn(d)
            return carry
        lax.fori_loop(1, ny, step, 0)

    loop_peers(lambda d: to_peer(d, 1).start())
    to_sib(tm, 1).start()

    for p, there in ((0, has_above), (2, has_below)):
        @pl.when(there)
        def _(p=p):
            from_any(tm, p).wait_recv()
            loop_peers(lambda d: to_peer(d, p).start())
            to_sib(tm, p).start()

    pltpu.make_async_remote_copy(
        src_ref=stats.at[pl.ds(0, total - 1)], dst_ref=stats.at[pl.ds(0, total - 1)],
        send_sem=stat_send, recv_sem=stat_recv, device_id=(sib, row),
        device_id_type=MESH).wait()
    every = stats[...].reshape(total, LANES)
    summed = jnp.sum(every, axis=0, keepdims=True)
    middle = summed * (1.0 / total)
    away = every - middle
    away = jnp.sum(away * away, axis=0, keepdims=True) * count
    rows = []
    for i in range(chunks):
        rows.append(jnp.where(place == i, middle, 0.0))
    for i in range(chunks):
        rows.append(jnp.where(place == chunks + i, summed, 0.0)
                    + jnp.where(place == i, away, 0.0))
    spread_out = group_sum(jnp.concatenate(rows, axis=0), span)
    center = jnp.concatenate([spread_out[i:i + 1] for i in range(chunks)], axis=1)
    spread = jnp.concatenate(
        [spread_out[chunks + i:chunks + i + 1] for i in range(chunks)], axis=1)
    spread = spread * (1.0 / (count * total))
    gain = lax.rsqrt(spread + EPSILON) * gamma[...]
    shift = beta[...]

    column = lax.broadcasted_iota(jnp.int32, (across, channels), 0)

    def activate_row(f, i, there=None):
        v = (raw[f, i].astype(jnp.float32) - center) * gain + shift
        v = v * 0.5
        v = v * jnp.tanh(v) + v
        if there is not None:
            v = jnp.where(there, v, 0.0)
        before = jnp.where(column == 0, 0.0, pltpu.roll(v, 1, 0))
        after = jnp.where(column == across - 1, 0.0, pltpu.roll(v, across - 1, 0))
        xs[f, i, :, 0:channels] = before.astype(jnp.bfloat16)
        xs[f, i, :, channels:2 * channels] = v.astype(jnp.bfloat16)
        xs[f, i, :, 2 * channels:] = after.astype(jnp.bfloat16)

    def activate(f):
        activate_row(f, 0, has_above)
        for i in range(1, height + 1):
            activate_row(f, i)
        activate_row(f, height + 1, has_below)

    def dot(base, taps):
        total_out = None
        for b in range(3):
            left = xs[pl.ds(base, CORES), b:b + height]
            left = left.reshape(CORES * height * across, 3 * channels)
            part = lax.dot_general(left, taps[b], (((1,), (1,)), ((), ())),
                                   preferred_element_type=jnp.float32)
            total_out = part if total_out is None else total_out + part
        return total_out.reshape(CORES, height, across, -1)

    def convolve(base):
        pair = dot(base, wp)
        prod[1, pl.ds(base, CORES)] = pair[..., 0:outs]
        prod[2, pl.ds(base, CORES)] = pair[..., outs:2 * outs]

        @pl.when(jnp.logical_or(base == 0, base + 2 < nt))
        def _():
            prod[0, pl.ds(base, CORES)] = dot(base, w0)

    def wait_frame(f, forward):
        from_any(f, 1).wait_recv()
        if forward:
            to_sib(f, 1).start()
        for p, there in ((0, has_above), (2, has_below)):
            @pl.when(there)
            def _(p=p):
                from_any(f, p).wait_recv()
                if forward:
                    to_sib(f, p).start()

    pltpu.make_async_copy(w0, w0, w_sem.at[0]).wait()
    pltpu.make_async_copy(wp, wp, w_sem.at[1]).wait()
    activate(tm)
    wait_frame(sib, False)
    activate(sib)
    convolve(y * CORES)

    def far(d):
        base = lax.rem(y + d, ny) * CORES
        wait_frame(base + core, True)
        activate(base + core)
        wait_frame(base + 1 - core, False)
        activate(base + 1 - core)
        convolve(base)

    loop_peers(far)

    direct = outs % LANES == 0

    def lanes_of(x):
        if direct:
            return x[..., pl.ds(pl.multiple_of(tm * outs, LANES), outs)]
        full = x[...].astype(jnp.float32)
        lead = full.shape[:-1]
        moved = pltpu.roll(full.reshape(-1, channels), channels - tm * outs, 1)
        return moved[:, 0:outs].reshape(*lead, outs)

    if direct:
        offset = lanes_of(bias)
    else:
        offset = lanes_of(jnp.broadcast_to(bias[...], (8, channels)))[0:1]

    def landing(src):
        if direct:
            return out.at[0, :, :, pl.ds(pl.multiple_of(src * outs, LANES), outs)]
        return out.at[src]

    def out_copy(f):
        return pltpu.make_async_remote_copy(
            src_ref=block.at[f], dst_ref=landing(tm), send_sem=out_send.at[f],
            recv_sem=out_recv.at[tm], device_id=(f, row), device_id_type=MESH)

    def finish(f):
        conv = (prod[2, f] + prod[1, jnp.maximum(f - 1, 0)]) + prod[0, jnp.maximum(f - 2, 0)]
        kept = lanes_of(raw.at[f, 1:1 + height]).astype(jnp.float32)
        return (kept + conv + offset).astype(jnp.bfloat16)

    def give(f):
        block[f] = finish(f)
        out_copy(f).start()

    def give_far(d):
        base = lax.rem(y + d, ny) * CORES
        give(base + core)
        give(base + 1 - core)

    loop_peers(give_far)
    give(sib)
    block[tm] = finish(tm)
    keep = pltpu.make_async_copy(block.at[tm], landing(tm), feat_sem)
    keep.start()

    def take(i, carry):
        src = lax.rem(tm + i, nt)
        pltpu.make_async_remote_copy(
            src_ref=block.at[src], dst_ref=landing(src), send_sem=out_send.at[src],
            recv_sem=out_recv.at[src], device_id=(sib, row), device_id_type=MESH).wait()
        return carry

    lax.fori_loop(1, nt, take, 0)
    keep.wait()

    @pl.when(has_below)
    def _():
        up_copy.wait_send()

    @pl.when(has_above)
    def _():
        down_copy.wait_send()

    for p, there in ((0, has_above), (1, None), (2, has_below)):
        def drain(p=p):
            def one(d):
                to_peer(d, p).wait_send()
                to_sib(lax.rem(y + d, ny) * CORES + core, p).wait_send()
            loop_peers(one)
            to_sib(tm, p).wait_send()
        if there is None:
            drain()
        else:
            pl.when(there)(drain)


def local(nt, nr, features, gamma, beta, kernel, bias):
    _, height, across, channels = features.shape
    outs = kernel.shape[1]
    total = nt * nr
    weights = jnp.transpose(kernel, (0, 2, 3, 1, 4))
    direct = outs % LANES == 0
    shape = features.shape if direct else (nt, height, across, outs)
    vmem = pl.BlockSpec(memory_space=pltpu.VMEM)
    hbm = pl.BlockSpec(memory_space=pltpu.HBM)
    bf16, f32 = jnp.bfloat16, jnp.float32
    dma = pltpu.SemaphoreType.DMA
    parts = pl.pallas_call(
        functools.partial(body, nt, nr),
        out_shape=jax.ShapeDtypeStruct(shape, bf16),
        in_specs=[hbm, vmem, vmem, hbm, vmem],
        out_specs=pl.BlockSpec(memory_space=pl.ANY),
        scratch_shapes=[
            pltpu.VMEM((nt, height + 2, across, channels), bf16),
            pltpu.VMEM((nt, height + 2, across, 3 * channels), bf16),
            pltpu.VMEM((3, 2 * outs, 3 * channels), bf16),
            pltpu.VMEM((3, outs, 3 * channels), bf16),
            pltpu.VMEM((3, nt, height, across, outs), f32),
            pltpu.VMEM((total, 1, LANES), f32),
            pltpu.VMEM((nt, height, across, outs), bf16),
            dma, dma((2,)), dma, dma,
            dma((2,)), dma((nt, 3)), dma((nt // CORES, 3)), dma((nt, 3)),
            dma((nt,)), dma((nt,)),
        ],
        compiler_params=pltpu.CompilerParams(collective_id=0, has_side_effects=True,
                                             vmem_limit_bytes=VMEM_LIMIT),
    )(features, gamma.reshape(1, -1), beta.reshape(1, -1), weights, bias.reshape(1, -1))
    if direct:
        return parts
    return jnp.transpose(parts, (1, 2, 0, 3)).reshape(features.shape)


def solution(mesh):
    nt, nr = mesh.shape["tm"], mesh.shape["rows"]
    in_specs = (P("tm", "rows", None, None), P(), P(), P(None, "tm", None, None, None), P())
    out_specs = P("tm", "rows", None, None)
    return jax.shard_map(functools.partial(local, nt, nr), mesh=mesh, in_specs=in_specs,
                         out_specs=out_specs, check_vma=False)
```
